32 devices in a mesh: blk: 32 (over z, y, x, core).
Axes of the slice: x: 2, y: 2, z: 4, core: 2. Of those that a mesh axis runs over, the one named last changes fastest.
Arguments:
- adjacency: int32 [8192, 1280], P('blk'), may hold values 0 or 1
- weight: bfloat16 [8192, 1280], P('blk'), may hold values from -6 to 6
Outputs:
- closure: float32 [8192, 4352], P('blk')
The draws below stay inside these ranges and needn't reach their ends.
All inputs are finite; a program needn't handle non-finite values. No bound on the sum of `adjacency` on one device may be relied on, other than what follows from the above.
Results may differ from the reference program's by a relative error of at most 0.0041.
Values may be sent and summed in bfloat16 or wider, within the bound.
A program may use at most 64 MiB of HBM per device.

```python
import math
import jax
import jax.numpy as jnp
from jax import lax

B = 512
R = 256
K = 2
N = 8192


def place_ends(array, stream_key, least, largest):
    index_at = [jax.random.randint(jax.random.fold_in(stream_key, axis), (), 0, length) for axis, length in enumerate(array.shape)]
    main_axis = array.shape.index(max(array.shape))
    next_to = index_at[:main_axis] + [(index_at[main_axis] + 1) % array.shape[main_axis]] + index_at[main_axis + 1:]
    return array.at[tuple(index_at)].set(least).at[tuple(next_to)].set(largest)


def block_levels(own_key, shape, cuts, smallest, high):
    def one(dim, blocks):
        steps = jax.random.uniform(jax.random.fold_in(jax.random.fold_in(own_key, 6), dim), (blocks,), jnp.float32, smallest / len(cuts), high / len(cuts))
        return jnp.repeat(jnp.exp(steps), shape[dim] // blocks).reshape((-1,) + (1,) * (len(shape) - dim - 1))

    factor_of = one(*cuts[0])
    for cut in cuts[1:]:
        factor_of = factor_of * one(*cut)
    return factor_of


def noise(own_key, shape, scale, most, pieces=(), dtype=jnp.bfloat16):
    values = jax.random.normal(own_key, shape, jnp.float32) * scale
    if len(pieces) > 0:
        values = block_levels(own_key, shape, pieces, -0.22, 0.18) * values
    return jnp.clip(values, min=-most, max=most).astype(dtype)


def setup_inputs(seed: int = 0) -> dict:
    streams_of = jax.random.split(jax.random.key(seed), 3)
    return {
        "adjacency": place_ends((jax.random.randint(streams_of[0], (N, (2 * K + 1) * R), 0, 2) < 1).astype(jnp.int32), jax.random.fold_in(streams_of[0], 1), 0, 1),
        "weight": noise(streams_of[1], (N, (2 * K + 1) * R), 1.0, 6.0, ((0, 32),)),
    }


def banded(adjacency, weight):
    reach = (adjacency.shape[1] // R - 1) // 2
    local_row = lax.broadcasted_iota(jnp.int32, adjacency.shape, 0) % R
    offset = lax.broadcasted_iota(jnp.int32, adjacency.shape, 1) - local_row - reach * R
    keep = (jnp.abs(offset) <= B) & ((adjacency == 1) | (offset == 0))
    return jnp.where(keep, weight, jnp.zeros_like(weight))

def square(matrix, scale):
    block_count = matrix.shape[0] // R
    width_cols = matrix.shape[1]
    reach = (width_cols // R - 1) // 2
    blocks = matrix.reshape(block_count, R, width_cols)
    result = jnp.zeros((block_count, R, (4 * reach + 1) * R), jnp.float32)
    for column in range(2 * reach + 1):
        neighbour = jnp.roll(blocks, -(column - reach), axis=0).astype(jnp.float32)
        left = blocks[:, :, column * R:(column + 1) * R].astype(jnp.float32)
        product = jnp.einsum('bij,bjk->bik', left, neighbour)
        result = result.at[:, :, column * R:column * R + width_cols].add(product)
    return (result * scale).reshape(block_count * R, (4 * reach + 1) * R)

def reference(adjacency, weight):
    matrix = banded(adjacency, weight)
    first = square(matrix, 1.0 / math.sqrt(B)).astype(jnp.bfloat16)
    return square(first, 1.0 / math.sqrt(2 * B))
```

```python
import functools
import math

import jax
import jax.numpy as jnp
from jax import lax
from jax.experimental import pallas as pl
from jax.experimental.pallas import tpu as pltpu
from jax.sharding import PartitionSpec as P

B = 512
MESH = pl.DeviceIdType.MESH
CORES = 2
PLANE = 4
SPAN = PLANE - 1
PAD = 16
CHUNKS = 4


def banded(adjacency, weight):
    row_count = adjacency.shape[0]
    reach = (adjacency.shape[1] // row_count - 1) // 2
    local_row = lax.broadcasted_iota(jnp.int32, adjacency.shape, 0)
    offset = lax.broadcasted_iota(jnp.int32, adjacency.shape, 1) - local_row - reach * row_count
    keep = (jnp.abs(offset) <= B) & ((adjacency == 1) | (offset == 0))
    return jnp.where(keep, weight, jnp.zeros_like(weight))


def pack(matrix):
    rows = matrix.shape[0]
    first, last = matrix[:, :rows], matrix[:, -rows:]
    r = lax.broadcasted_iota(jnp.int32, (rows, rows), 0)
    c = lax.broadcasted_iota(jnp.int32, (rows, rows), 1)
    square = jnp.where(c >= r, first, last)
    diagonal = jnp.sum(jnp.where(c == r, last, 0).astype(jnp.float32), axis=0, keepdims=True)
    diagonal = jnp.pad(diagonal.astype(matrix.dtype), ((0, PAD - 1), (0, matrix.shape[1] - 2 * rows)))
    body = jnp.concatenate([square, matrix[:, rows:-rows]], axis=1)
    return jnp.concatenate([body, diagonal], axis=0)


def kernel(
    n, rows, packed, out, buf, first, last, p_acc, t_acc, p_low, t_low,
    own_send, pair_send, hop_send, recv, local_sem,
):
    me = lax.axis_index("blk")
    core = me % CORES
    place = (me // CORES) % PLANE
    group = me // (CORES * PLANE)
    groups = n // (CORES * PLANE)
    partner = me + 1 - 2 * core
    up = ((group + 1) % groups * PLANE + place) * CORES + core
    down = ((group + groups - 1) % groups * PLANE + place) * CORES + core
    mates = (SPAN - place, (place + 2) % PLANE, place + 1 - 2 * (place % 2))

    def device(q):
        return (group * PLANE + q) * CORES + core

    def slot(chip_offset, c):
        return (chip_offset + SPAN) * CORES + c

    total = rows + PAD
    step = rows // CHUNKS
    bounds = [(j * step, step if j < CHUNKS - 1 else total - j * step) for j in range(CHUNKS)]

    barrier = pltpu.get_barrier_semaphore()
    greeted = [partner, up, down] + [device(q) for q in mates]
    for other in greeted:
        pl.semaphore_signal(barrier, inc=1, device_id=(other,), device_id_type=MESH)
    pl.semaphore_wait(barrier, len(greeted))

    def chunk(ref, j):
        return ref.at[pl.ds(bounds[j][0], bounds[j][1])]

    def own(index, j, to, at):
        return pltpu.make_async_remote_copy(
            src_ref=chunk(packed, j),
            dst_ref=chunk(buf.at[at], j),
            send_sem=own_send.at[index, j],
            recv_sem=recv.at[at, j],
            device_id=(to,),
            device_id_type=MESH,
        )

    def forward(sem, source, j, to, at):
        return pltpu.make_async_remote_copy(
            src_ref=chunk(buf.at[source], j),
            dst_ref=chunk(buf.at[at], j),
            send_sem=sem,
            recv_sem=recv.at[at, j],
            device_id=(to,),
            device_id_type=MESH,
        )

    def arrived(at, j):
        pltpu.make_async_copy(chunk(packed, j), chunk(buf.at[at], j), recv.at[at, j]).wait()

    sent = []

    def go(copy):
        copy.start()
        sent.append(copy)

    for j in range(CHUNKS):
        for index in (0, 1):
            go(own(index, j, device(mates[index]), slot(place - mates[index], core)))
    for j in range(CHUNKS):
        go(own(2, j, device(mates[2]), slot(place - mates[2], core)))
        go(own(3, j, partner, slot(0, core)))
    mine = pltpu.make_async_copy(packed, buf.at[slot(0, core)], local_sem)
    mine.start()
    p_acc[...] = jnp.zeros_like(p_acc)
    t_acc[...] = jnp.zeros_like(t_acc)
    out[...] = jnp.zeros_like(out)

    def mate_in(index, j):
        q = mates[index]
        at = slot(q - place, core)
        arrived(at, j)
        above = (q - place + PLANE) // PLANE
        target = above * up + (1 - above) * down
        there = slot(q - place + PLANE - 2 * PLANE * above, core)
        go(forward(hop_send.at[index, j], at, j, target, there))
        go(forward(pair_send.at[index, j], at, j, partner, at))

    def relay_slot(index, c):
        q = mates[index]
        above = (q - place + PLANE) // PLANE
        return slot(q - place + PLANE - 2 * PLANE * above, c)

    def relay_in(index, j):
        at = relay_slot(index, core)
        arrived(at, j)
        go(forward(pair_send.at[3 + index, j], at, j, partner, at))

    def other_in(at):
        for j in range(CHUNKS):
            arrived(at, j)

    def unpack(at):
        square = buf[at, :rows, :rows]
        r = lax.broadcasted_iota(jnp.int32, (rows, rows), 0)
        c = lax.broadcasted_iota(jnp.int32, (rows, rows), 1)
        diagonal = buf[at, rows : rows + 1, :rows]
        zero = jnp.zeros_like(square)
        first[at] = jnp.where(c >= r, square, zero)
        last[at] = jnp.where(c < r, square, jnp.where(c == r, diagonal, zero))

    middle = 3 * rows

    def unit(left, at, acc, column):
        begin = pl.multiple_of(column * rows, rows)
        for ref, start, width in (
            (first.at[at], 0, rows),
            (buf.at[at, pl.ds(0, rows), pl.ds(rows, middle)], rows, middle),
            (last.at[at], rows + middle, rows),
        ):
            where = pl.ds(pl.multiple_of(begin + start, rows), width)
            acc[:, where] += jnp.dot(left, ref[...], preferred_element_type=jnp.float32)

    for j in range(CHUNKS):
        mate_in(0, j)
        mate_in(1, j)
    for j in range(CHUNKS):
        mate_in(2, j)
        relay_in(0, j)
        relay_in(1, j)
    mine.wait()
    other_in(slot(0, 1 - core))
    for index in range(3):
        other_in(slot(mates[index] - place, 1 - core))
    for index in (0, 1):
        other_in(relay_slot(index, 1 - core))
    for j in range(CHUNKS):
        relay_in(2, j)
    other_in(relay_slot(2, 1 - core))

    def unpack_all(b, carry):
        unpack(b)
        return carry

    lax.fori_loop(0, (2 * SPAN + 1) * CORES, unpack_all, 0)

    center = slot(0, core)
    lefts = (
        [first[center]]
        + [buf[center, :rows, (1 + m) * rows : (2 + m) * rows] for m in range(3)]
        + [last[center]]
    )
    for t in range(5):
        unit(lefts[t], center - 2 + t, p_acc, t)
    p_low[...] = (p_acc[...] * (1.0 / math.sqrt(B))).astype(p_low.dtype)

    def second(t, carry):
        left = p_low[:, pl.ds(pl.multiple_of(t * rows, rows), rows)]
        unit(left, center - 4 + t, t_acc, t)
        return carry

    lax.fori_loop(0, 9, second, 0)
    scale = 1.0 / math.sqrt(B) / math.sqrt(2 * B)
    t_low[...] = (t_acc[...] * scale).astype(t_low.dtype)

    def third(t, carry):
        left = t_low[:, pl.ds(pl.multiple_of(t * rows, rows), rows)]
        unit(left, center - 6 + t, out, t)
        return carry

    lax.fori_loop(0, 13, third, 0)
    for copy in sent:
        copy.wait_send()


def local(n, adjacency, weight):
    rows = adjacency.shape[0]
    packed = pack(banded(adjacency, weight))
    wide = packed.shape[1]
    slots = (2 * SPAN + 1) * CORES
    low = packed.dtype
    return pl.pallas_call(
        functools.partial(kernel, n, rows),
        out_shape=jax.ShapeDtypeStruct((rows, 17 * rows), jnp.float32),
        in_specs=[pl.BlockSpec(memory_space=pltpu.VMEM)],
        out_specs=pl.BlockSpec(memory_space=pltpu.VMEM),
        scratch_shapes=[
            pltpu.VMEM((slots, rows + PAD, wide), low),
            pltpu.VMEM((slots, rows, rows), low),
            pltpu.VMEM((slots, rows, rows), low),
            pltpu.VMEM((rows, 9 * rows), jnp.float32),
            pltpu.VMEM((rows, 13 * rows), jnp.float32),
            pltpu.VMEM((rows, 9 * rows), low),
            pltpu.VMEM((rows, 13 * rows), low),
            pltpu.SemaphoreType.DMA((4, CHUNKS)),
            pltpu.SemaphoreType.DMA((6, CHUNKS)),
            pltpu.SemaphoreType.DMA((3, CHUNKS)),
            pltpu.SemaphoreType.DMA((slots, CHUNKS)),
            pltpu.SemaphoreType.DMA,
        ],
        compiler_params=pltpu.CompilerParams(
            collective_id=0, has_side_effects=True, vmem_limit_bytes=56 * 1024 * 1024
        ),
    )(packed)


def solution(mesh):
    in_specs = (P("blk", None), P("blk", None))
    out_specs = P("blk", None)
    n = mesh.shape["blk"]
    return jax.shard_map(
        functools.partial(local, n), mesh=mesh, in_specs=in_specs, out_specs=out_specs, check_vma=False
    )
```

```python
import functools
import math

import jax
import jax.numpy as jnp
from jax import lax
from jax.experimental import pallas as pl
from jax.experimental.pallas import tpu as pltpu
from jax.sharding import PartitionSpec as P

B = 512
MESH = pl.DeviceIdType.MESH
CORES = 2
PLANE = 4
SPAN = PLANE - 1
PAD = 16
CHUNKS = 4


def banded(adjacency, weight):
    row_count = adjacency.shape[0]
    reach = (adjacency.shape[1] // row_count - 1) // 2
    local_row = lax.broadcasted_iota(jnp.int32, adjacency.shape, 0)
    offset = lax.broadcasted_iota(jnp.int32, adjacency.shape, 1) - local_row - reach * row_count
    keep = (jnp.abs(offset) <= B) & ((adjacency == 1) | (offset == 0))
    return jnp.where(keep, weight, jnp.zeros_like(weight))


def pack(matrix):
    rows = matrix.shape[0]
    first, last = matrix[:, :rows], matrix[:, -rows:]
    r = lax.broadcasted_iota(jnp.int32, (rows, rows), 0)
    c = lax.broadcasted_iota(jnp.int32, (rows, rows), 1)
    square = jnp.where(c >= r, first, last)
    diagonal = jnp.sum(jnp.where(c == r, last, 0).astype(jnp.float32), axis=0, keepdims=True)
    diagonal = jnp.pad(diagonal.astype(matrix.dtype), ((0, PAD - 1), (0, matrix.shape[1] - 2 * rows)))
    body = jnp.concatenate([square, matrix[:, rows:-rows]], axis=1)
    return jnp.concatenate([body, diagonal], axis=0)


def kernel(
    n, rows, packed, out, buf, cols, row, p_low, t_low,
    own_send, pair_send, hop_send, side_send, recv, local_sem,
):
    me = lax.axis_index("blk")
    core = me % CORES
    place = (me // CORES) % PLANE
    group = me // (CORES * PLANE)
    groups = n // (CORES * PLANE)
    partner = me + 1 - 2 * core
    up = ((group + 1) % groups * PLANE + place) * CORES + core
    down = ((group + groups - 1) % groups * PLANE + place) * CORES + core
    x_mate = place + 1 - 2 * (place % 2)
    y_mate = (place + 2) % PLANE
    inner = (place + 1) // 2 % 2
    a_mate = (1 - inner) * x_mate + inner * y_mate
    b_mate = inner * x_mate + (1 - inner) * y_mate
    d_mate = SPAN - place

    def device(q):
        return (group * PLANE + q) * CORES + core

    def slot(chip_offset, c):
        return (chip_offset + SPAN) * CORES + c

    def is_above(q, p):
        return (q - p + PLANE) // PLANE

    def cross(q, p):
        return q - p + PLANE - 2 * PLANE * is_above(q, p)

    total = rows + PAD
    step = rows // CHUNKS
    bounds = [(j * step, step if j < CHUNKS - 1 else total - j * step) for j in range(CHUNKS)]

    barrier = pltpu.get_barrier_semaphore()
    greeted = [partner, up, down, device(a_mate), device(b_mate)]
    for other in greeted:
        pl.semaphore_signal(barrier, inc=1, device_id=(other,), device_id_type=MESH)
    pl.semaphore_wait(barrier, len(greeted))

    def chunk(ref, j):
        return ref.at[pl.ds(bounds[j][0], bounds[j][1])]

    sent = []

    def send(source, sem, j, to, at):
        copy = pltpu.make_async_remote_copy(
            src_ref=chunk(source, j),
            dst_ref=chunk(buf.at[at], j),
            send_sem=sem,
            recv_sem=recv.at[at, j],
            device_id=(to,),
            device_id_type=MESH,
        )
        copy.start()
        sent.append(copy)

    def arrived(at, j):
        pltpu.make_async_copy(chunk(packed, j), chunk(buf.at[at], j), recv.at[at, j]).wait()

    def pair(index, at, j):
        send(buf.at[at], pair_send.at[index, j], j, partner, at)

    def hop(index, q, j):
        above = is_above(q, place)
        to = above * up + (1 - above) * down
        send(buf.at[slot(q - place, core)], hop_send.at[index, j], j, to, slot(cross(q, place), core))

    center = slot(0, core)
    a_in, b_in, d_in = (slot(q - place, core) for q in (a_mate, b_mate, d_mate))
    a_far, b_far, d_far = (slot(cross(q, place), core) for q in (a_mate, b_mate, d_mate))

    for j in range(CHUNKS):
        send(packed, own_send.at[0, j], j, device(b_mate), slot(place - b_mate, core))
        send(packed, own_send.at[1, j], j, device(a_mate), slot(place - a_mate, core))
    mine = pltpu.make_async_copy(packed, buf.at[center], local_sem)
    mine.start()
    for j in range(CHUNKS):
        send(packed, own_send.at[2, j], j, partner, center)

    r = lax.broadcasted_iota(jnp.int32, (rows, rows), 0)
    c = lax.broadcasted_iota(jnp.int32, (rows, rows), 1)

    def triangles(at):
        square = buf[at, :rows, :rows]
        diagonal = buf[at, rows : rows + 1, :rows]
        zero = jnp.zeros_like(square)
        return (
            jnp.where(c >= r, square, zero),
            jnp.where(c < r, square, jnp.where(c == r, diagonal, zero)),
        )

    def unpack(at):
        first, last = triangles(at)
        cols[at, 4 * rows : 5 * rows, :] = first
        for k in range(1, 4):
            cols[at + k, (4 - k) * rows : (5 - k) * rows, :] = buf[at, :rows, k * rows : (k + 1) * rows]
        cols[at + 4, :rows, :] = last

    def take_other(at):
        other = at + 1 - 2 * core
        for j in range(CHUNKS):
            arrived(other, j)
        unpack(other)

    for j in range(CHUNKS):
        arrived(b_in, j)
        hop(0, b_mate, j)
        pair(0, b_in, j)
        arrived(a_in, j)
        send(buf.at[a_in], side_send.at[0, j], j, device(b_mate), slot(a_mate - b_mate, core))
        pair(1, a_in, j)
    for j in range(CHUNKS):
        hop(1, a_mate, j)
    for j in range(CHUNKS):
        arrived(b_far, j)
        send(
            buf.at[b_far], side_send.at[1, j], j, device(a_mate),
            slot(cross(b_mate, place) + place - a_mate, core),
        )
        pair(2, b_far, j)
    mine.wait()
    first, last = triangles(center)
    row[:, :rows] = first
    row[:, rows : 4 * rows] = buf[center, :rows, rows:]
    row[:, 4 * rows :] = last
    for at in (center, a_in, b_in, b_far):
        unpack(at)
    for at in (center, a_in, b_in):
        take_other(at)
    for j in range(CHUNKS):
        arrived(d_in, j)
        pair(3, d_in, j)
        arrived(a_far, j)
        pair(4, a_far, j)
        arrived(d_far, j)
        pair(5, d_far, j)
    for at in (d_in, a_far, d_far):
        unpack(at)
    for at in (b_far, d_in, a_far, d_far):
        take_other(at)

    def product(left, least, most, column):
        low, high = max(least, column - 4), min(most, column)
        return jnp.dot(
            left[:, (low - least) * rows : (high + 1 - least) * rows],
            cols[column + core, (low - column + 4) * rows : (high - column + 5) * rows, :],
            preferred_element_type=jnp.float32,
        )

    for u in range(9):
        p_low[:, u * rows : (u + 1) * rows] = (
            product(row, 4, 8, u + 4) * (1.0 / math.sqrt(B))
        ).astype(p_low.dtype)
    scale = 1.0 / math.sqrt(B) / math.sqrt(2 * B)
    for u in range(13):
        t_low[:, u * rows : (u + 1) * rows] = (product(p_low, 2, 10, u + 2) * scale).astype(t_low.dtype)
    for u in range(17):
        out[:, u * rows : (u + 1) * rows] = product(t_low, 0, 12, u)
    for copy in sent:
        copy.wait_send()


def local(n, adjacency, weight):
    rows = adjacency.shape[0]
    packed = pack(banded(adjacency, weight))
    wide = packed.shape[1]
    slots = (2 * SPAN + 1) * CORES
    low = packed.dtype
    return pl.pallas_call(
        functools.partial(kernel, n, rows),
        out_shape=jax.ShapeDtypeStruct((rows, 17 * rows), jnp.float32),
        in_specs=[pl.BlockSpec(memory_space=pltpu.VMEM)],
        out_specs=pl.BlockSpec(memory_space=pltpu.VMEM),
        scratch_shapes=[
            pltpu.VMEM((slots, rows + PAD, wide), low),
            pltpu.VMEM((slots + 4, 5 * rows, rows), low),
            pltpu.VMEM((rows, 5 * rows), low),
            pltpu.VMEM((rows, 9 * rows), low),
            pltpu.VMEM((rows, 13 * rows), low),
            pltpu.SemaphoreType.DMA((3, CHUNKS)),
            pltpu.SemaphoreType.DMA((6, CHUNKS)),
            pltpu.SemaphoreType.DMA((2, CHUNKS)),
            pltpu.SemaphoreType.DMA((2, CHUNKS)),
            pltpu.SemaphoreType.DMA((slots, CHUNKS)),
            pltpu.SemaphoreType.DMA,
        ],
        compiler_params=pltpu.CompilerParams(
            collective_id=0, has_side_effects=True, vmem_limit_bytes=40 * 1024 * 1024
        ),
    )(packed)


def solution(mesh):
    in_specs = (P("blk", None), P("blk", None))
    out_specs = P("blk", None)
    n = mesh.shape["blk"]
    return jax.shard_map(
        functools.partial(local, n), mesh=mesh, in_specs=in_specs, out_specs=out_specs, check_vma=False
    )
```
